1024 devices in a mesh: dp: 32 (over z_lo, x), expert: 32 (over z_hi, y, core).
Axes of the slice: x: 4, y: 4, z: 32 (z_hi: 4, z_lo: 8; z = z_hi * 8 + z_lo), core: 2. Of those that a mesh axis runs over, the one named last changes fastest.
Arguments:
- hidden: bfloat16 [131072, 1024], P(('dp', 'expert')), may hold values from -6 to 6
- grad_out: bfloat16 [131072, 1024], P(('dp', 'expert')), may hold values from -48 to 48
- router_weight: float32 [1024, 32], replicated, may hold values from -0.1875 to 0.1875
- expert_ids: int32 [131072, 6], P(('dp', 'expert')), may hold values from 0 to 31, all different within a row; in each aligned block of 64 rows (0 to 63, 64 to 127, ...) at most 13 rows name the same one
- pre_gate: bfloat16 [32, 32, 832, 704], P('dp', 'expert'), may hold values from -6 to 6
- pre_up: bfloat16 [32, 32, 832, 704], P('dp', 'expert'), may hold values from -6 to 6
- w_gate: bfloat16 [32, 1024, 704], P('expert'), may hold values from -0.1875 to 0.1875
- w_up: bfloat16 [32, 1024, 704], P('expert'), may hold values from -0.1875 to 0.1875
- w_down: bfloat16 [32, 704, 1024], P('expert'), may hold values from -0.21875 to 0.21875
Outputs:
- grad_x: bfloat16 [131072, 1024], P(('dp', 'expert'))
- router_update: float32 [1024, 32], P('dp', 'expert')
The draws below stay inside these ranges and needn't reach their ends.
Inputs may be any that keep to these rules, and one draw needn't show every extreme that they name: `expert_ids`: each row names 6 different experts; in each aligned block of 64 rows no expert is named by more than 13 rows.
All inputs are finite; a program needn't handle non-finite values.
Results may differ from the reference program's by a relative error of at most 0.006.
Values may be sent and summed in bfloat16 or wider, within the bound.
A program may use at most 32 MiB of HBM per device.

```python
import math
import jax
import jax.numpy as jnp
import numpy as np
from jax import lax

D = 1024
FF = 704
TOK_DEV = 128
BLK = 64
EXPERTS = 32
TOP = 6
CAP = 13
TOKENS = 131072
N_DP = 32
N_EXPERT = 32


def levels(key, shape, cuts, smallest, top_value):
    level = 1.0
    for axis_at, shards_of in cuts:
        heights = jax.random.uniform(jax.random.fold_in(jax.random.fold_in(key, 6), axis_at), (shards_of,), jnp.float32, smallest / len(cuts), top_value / len(cuts))
        level = level * jnp.repeat(jnp.exp(heights), shape[axis_at] // shards_of).reshape((-1,) + (1,) * (len(shape) - 1 - axis_at))
    return level


def routed_block(key, own, number, rows, count, top, most, lean):
    ranking = jax.random.permutation(key, count)
    heavy_load, usual = shares(count, rows * top, most, lean, True), shares(count, rows * top, most, lean, False)
    places = jnp.arange(count)

    def named(sizes, turn):
        used = int((sizes > 0).sum())
        fixed = max(1, used // 4)
        moved = fixed + (places - fixed + turn * (used - fixed)) % max(1, count - fixed)
        return jnp.zeros((count,), jnp.int32).at[ranking[jnp.where(places < fixed, places, moved)]].set(jnp.asarray(sizes, jnp.int32))

    sizes = jnp.where(number % 4 == 0, named(heavy_load, number // 4), named(usual, number - number // 4 - 1))
    mixed = jax.random.permutation(jax.random.fold_in(own, 3), count)
    donor, taker = mixed[0:count // 2 * 2:2], mixed[1:count // 2 * 2:2]
    margin = jnp.minimum(sizes[donor] - 1, most - sizes[taker]) // 2
    margin = jnp.where((donor == ranking[0]) | (taker == ranking[0]) | (sizes[taker] == 0), 0, jnp.maximum(margin, 0))
    moved = jax.random.randint(jax.random.fold_in(own, 4), (count // 2,), 0, 1 << 20) % (margin + 1)
    sizes = sizes.at[donor].add(-moved).at[taker].add(moved)
    labels = jnp.searchsorted(jnp.cumsum(sizes), jnp.arange(rows * top), side="right").astype(jnp.int32)
    table = labels.reshape(top, rows).T
    table = table[jax.random.permutation(jax.random.fold_in(own, 1), rows)]
    turn = jax.random.randint(jax.random.fold_in(own, 2), (rows, 1), 0, top)
    return jnp.take_along_axis(table, (jnp.arange(top)[None, :] + turn) % top, axis=1)


def shares(count, total, reach, slope, full):
    portions = [(1 << 20) // math.isqrt(grade ** slope) + 1 for grade in range(1, count + 1)]
    largest = reach if full else min(reach, max(-(-total // count), total * portions[0] // sum(portions)))
    least = 1 if total - largest >= count - 1 else 0
    given, rest = [largest] + [least] * (count - 1), total - largest - least * (count - 1)
    while rest > 0:
        movable = [i for i in range(1, count) if given[i] < largest] or [i for i in range(1, count) if given[i] < reach]
        pool, left = sum([portions[i] for i in movable]), rest
        for i in movable:
            extra = min(reach - given[i], max(1, left * portions[i] // pool), rest)
            given[i] = given[i] + extra
            rest = rest - extra
    return np.array(given)


def normal_values(own_key, dims, scale, bound, cuts=(), kind=jnp.bfloat16):
    factor_of = levels(own_key, dims, cuts, -0.22, 0.18) if cuts else 1.0
    array = jax.random.normal(own_key, dims, jnp.float32) * scale * factor_of
    return jnp.minimum(jnp.maximum(array, -bound), bound).astype(kind)


def setup_inputs(seed: int = 0) -> dict:
    seeds = jax.random.split(jax.random.key(seed), 10)
    hidden = normal_values(seeds[0], (TOKENS, D), 1.0, 6.0, ((0, 1024),))
    grad_out = normal_values(seeds[1], (TOKENS, D), 8.0, 48.0, ((0, 1024),))
    router_weight = normal_values(seeds[2], (D, EXPERTS), D ** -0.5, 0.1875, (), jnp.float32)
    expert_ids_keys = jax.random.split(jax.random.fold_in(seeds[3], 1), TOKENS // BLK)
    expert_ids_turns = jax.random.permutation(jax.random.fold_in(seeds[3], 3), TOKENS // BLK)
    expert_ids = jax.vmap(lambda own, number: routed_block(jax.random.fold_in(seeds[3], 2), own, number, BLK, EXPERTS, TOP, CAP, 2))(expert_ids_keys, expert_ids_turns).reshape((TOKENS, TOP))
    pre_gate = normal_values(seeds[4], (N_DP, EXPERTS, (TOK_DEV // BLK) * N_EXPERT * CAP, FF), 1.0, 6.0, ((0, 32), (1, 32)))
    pre_up = normal_values(seeds[5], (N_DP, EXPERTS, (TOK_DEV // BLK) * N_EXPERT * CAP, FF), 1.0, 6.0, ((0, 32), (1, 32)))
    w_gate = normal_values(seeds[6], (EXPERTS, D, FF), D ** -0.5, 0.1875, ((0, 32),))
    w_up = normal_values(seeds[7], (EXPERTS, D, FF), D ** -0.5, 0.1875, ((0, 32),))
    w_down = normal_values(seeds[8], (EXPERTS, FF, D), FF ** -0.5, 0.21875, ((0, 32),))
    return {"hidden": hidden, "grad_out": grad_out, "router_weight": router_weight, "expert_ids": expert_ids, "pre_gate": pre_gate, "pre_up": pre_up, "w_gate": w_gate, "w_up": w_up, "w_down": w_down}


PRECISE = lax.Precision.HIGHEST

def contract_last(left, right):
    return lax.dot_general(left, right, (((1,), (1,)), ((), ())), preferred_element_type=jnp.float32)

def slot_places(group_ids, block_rows, experts, capacity):
    tokens, top = group_ids.shape
    grouped = group_ids.reshape(tokens // block_rows, block_rows * top).astype(jnp.int32)
    hit_marks = (grouped[..., None] == jnp.arange(experts, dtype=jnp.int32)).astype(jnp.int32)
    earlier = jnp.cumsum(hit_marks, axis=1) - hit_marks
    slot_index = lax.optimization_barrier(jnp.sum(earlier * hit_marks, axis=-1)).astype(jnp.int32)
    flat_place = (grouped * capacity + slot_index).astype(jnp.int32)
    places = (flat_place[..., None] == jnp.arange(experts * capacity, dtype=jnp.int32)).astype(jnp.float32)
    return places.reshape(tokens // block_rows, block_rows, top, experts, capacity)

def expert_backward(sent_rows, gate_values, saved_gate, saved_up, w_gate, w_up, w_down):
    model_width = sent_rows.shape[-1]
    flat_rows = sent_rows.reshape(-1, model_width)
    dh_raw = contract_last(flat_rows, w_down)
    pre_first = saved_gate.reshape(-1, saved_gate.shape[-1]).astype(jnp.float32)
    pre_second = saved_up.reshape(-1, saved_up.shape[-1]).astype(jnp.float32)
    sigmoid_value = jax.nn.sigmoid(pre_first)
    active = pre_first * sigmoid_value
    slope_value = sigmoid_value * (1.0 + pre_first * (1.0 - sigmoid_value))
    gate_grad = lax.optimization_barrier(jnp.sum(dh_raw * active * pre_second, axis=-1))
    dh_scaled = gate_values.reshape(-1, 1).astype(jnp.float32) * dh_raw
    d_first = (dh_scaled * pre_second * slope_value).astype(jnp.bfloat16)
    d_second = (dh_scaled * active).astype(jnp.bfloat16)
    back_rows = contract_last(d_first, w_gate) + contract_last(d_second, w_up)
    return (back_rows.astype(jnp.bfloat16).reshape(sent_rows.shape), gate_grad.astype(jnp.bfloat16).reshape(sent_rows.shape[:-1]))

def reference(hidden, grad_out, router_weight, expert_ids, pre_gate, pre_up, w_gate, w_up, w_down):
    block_count = TOK_DEV // BLK
    model_width = hidden.shape[1]
    group_tokens = N_EXPERT * TOK_DEV
    logits = jnp.dot(hidden.astype(jnp.float32), router_weight, precision=PRECISE)
    exponent = jnp.exp(logits)
    probability = exponent / lax.optimization_barrier(jnp.sum(exponent, axis=-1, keepdims=True))
    picked = (expert_ids[..., None] == jnp.arange(EXPERTS, dtype=jnp.int32)).astype(jnp.float32)
    gate_values = lax.optimization_barrier(jnp.sum(picked * probability[:, None, :], axis=-1))

    def one_group(pieces):
        group_ids, cotangent, group_gates, saved_gate, saved_up = pieces
        places = slot_places(group_ids, BLK, EXPERTS, CAP).reshape(N_EXPERT, block_count, BLK, TOP, EXPERTS, CAP)
        chosen = lax.optimization_barrier(jnp.sum(places, axis=3))
        dense_rows = cotangent.reshape(N_EXPERT, block_count, BLK, model_width).astype(jnp.float32)
        sent_rows = jnp.einsum('snbec,snbd->enscd', chosen, dense_rows, precision=PRECISE).astype(jnp.bfloat16)
        sent_gate = jnp.einsum('snbkec,snbk->ensc', places, group_gates.reshape(N_EXPERT, block_count, BLK, TOP), precision=PRECISE).astype(jnp.bfloat16)
        saved_first = saved_gate.reshape(EXPERTS, block_count, N_EXPERT, CAP, saved_gate.shape[-1])
        saved_second = saved_up.reshape(EXPERTS, block_count, N_EXPERT, CAP, saved_up.shape[-1])

        def one_expert(items):
            return expert_backward(*items)
        back_rows, gate_grad = lax.map(one_expert, (sent_rows, sent_gate, saved_first, saved_second, w_gate, w_up, w_down))
        moe_part = jnp.einsum('snbec,enscd->snbd', chosen, back_rows.astype(jnp.float32), precision=PRECISE)
        gate_part = jnp.einsum('snbkec,ensc->snbk', places, gate_grad.astype(jnp.float32), precision=PRECISE)
        return (moe_part.reshape(group_tokens, model_width), gate_part.reshape(group_tokens, TOP))
    moe_grad, gate_grad = lax.map(one_group, (expert_ids.reshape(N_DP, group_tokens, TOP), grad_out.reshape(N_DP, group_tokens, model_width), gate_values.reshape(N_DP, group_tokens, TOP), pre_gate, pre_up))
    moe_grad = moe_grad.reshape(TOKENS, model_width)
    gate_grad = gate_grad.reshape(TOKENS, TOP)
    prob_grad = lax.optimization_barrier(jnp.sum(picked * gate_grad[..., None], axis=1))
    logit_grad = probability * (prob_grad - lax.optimization_barrier(jnp.sum(probability * prob_grad, axis=-1, keepdims=True)))
    grad_x = (moe_grad + jnp.dot(logit_grad, router_weight.T, precision=PRECISE)).astype(jnp.bfloat16)
    router_term = jnp.dot(hidden.astype(jnp.float32).T, logit_grad, precision=PRECISE)
    square_total = jnp.sum(router_term * router_term)
    factor = jnp.minimum(1.0, jnp.sqrt(model_width * EXPERTS / (square_total + 1e-06)))
    return (grad_x, router_term * factor)
```

```python
import jax
import jax.numpy as jnp
from jax import lax
from jax.experimental import pallas as pl
from jax.experimental.pallas import tpu as pltpu
from jax.sharding import Mesh
from jax.sharding import PartitionSpec as P

EXPERT = ("expert_0", "expert_1", "expert_2")
DP = ("dp_0", "dp_1")
DP_EXPERT = DP + EXPERT
PRECISE = lax.Precision.HIGHEST
F32 = jnp.float32
BF16 = jnp.bfloat16
WIDE = 1152


def dot(a, b, dims=((1,), (0,)), precision=None):
    return lax.dot_general(a, b, (dims, ((), ())), preferred_element_type=F32, precision=precision)


def iota(shape, dim):
    return lax.broadcasted_iota(jnp.int32, shape, dim)


def kernel(
    rows_ref, hidden_ref, rw_ref, rwt_ref, ids_ref, pre_gate_hbm, pre_up_hbm, wg_hbm, wu_hbm, wd_hbm,
    gx_ref, ru_ref,
    pre_gate, pre_up, wg, wu, wd, gathered, aux, aux_in, aux_relay,
    packed, arrived, back, returned, up_slope, act, act_up, probs,
    own_part, relay_part, comb_out, comb_mid, comb_in, pg_out, pg_relay, pg_all,
    terms, zl_in, stage_out, x_in, slab_in, zh_in, sq_out, sq_in, turned,
    local_sem, row_ss, row_rs, aux_ss, aux_rs, go_ss, go_rs, ret_ss, ret_rs,
    comb_ss, comb_rs, pg_ss, pg_rs, zl_ss, zl_rs, x_ss, x_rs, slab_ss, slab_rs, zh_ss, zh_rs, sq_ss, sq_rs,
):
    zl, x = lax.axis_index("dp_0"), lax.axis_index("dp_1")
    zh, y, c = (lax.axis_index(a) for a in EXPERT)
    yc = y * 2 + c
    up_z, down_z, far_z = lax.rem(zh + 1, 4), lax.rem(zh + 3, 4), lax.rem(zh + 2, 4)
    origin = (zh, down_z, up_z, far_z)
    sent = []

    def at_z(z):
        return {"expert_0": z}

    def at_slab(place):
        return {"expert_1": place // 2, "expert_2": lax.rem(place, 2)}

    def copy(src, dst, ss, rs, to):
        return pltpu.make_async_remote_copy(
            src_ref=src, dst_ref=dst, send_sem=ss, recv_sem=rs,
            device_id=to, device_id_type=pl.DeviceIdType.MESH,
        )

    def send(*args):
        made = copy(*args)
        made.start()
        sent.append(made)
        return made

    local = [
        pltpu.make_async_copy(src, dst, local_sem.at[i])
        for i, (src, dst) in enumerate(
            ((pre_gate_hbm, pre_gate), (pre_up_hbm, pre_up), (wd_hbm, wd), (wg_hbm, wg), (wu_hbm, wu))
        )
    ]
    for made in local:
        made.start()
    barrier = pltpu.get_barrier_semaphore()
    meet = [at_z(up_z), at_z(down_z)]
    meet += [at_slab(lax.rem(yc + d, 8)) for d in range(1, 8)]
    meet += [{"dp_0": lax.rem(zl + d, 8)} for d in range(1, 8)]
    meet += [{"dp_1": lax.rem(x + d, 4)} for d in range(1, 4)]
    for to in meet:
        pl.semaphore_signal(barrier, inc=1, device_id=to, device_id_type=pl.DeviceIdType.MESH)

    logits = dot(hidden_ref[...].astype(F32), rw_ref[...], precision=PRECISE)
    exponent = jnp.exp(logits.T[:32])
    probability = exponent / jnp.sum(exponent, axis=0, keepdims=True)
    probs[...] = probability
    ids = ids_ref[...]
    expert = iota((32, 128), 0)
    chosen = jnp.zeros((32, 128), F32)
    for k in range(6):
        chosen += jnp.where(expert == ids[k : k + 1], 1.0, 0.0)
    r, t = iota((128, 128), 0), iota((128, 128), 1)
    earlier = jnp.where((r < t) & ((r >> 6) == (t >> 6)), 1.0, 0.0).astype(BF16)
    slot = jnp.where(chosen > 0.5, dot(chosen.astype(BF16), earlier), -1.0)
    for b in range(4):
        aux[b] = jnp.concatenate([slot[8 * b : 8 * b + 8], probability[8 * b : 8 * b + 8]], axis=0).astype(BF16)
    pl.semaphore_wait(barrier, len(meet))

    first, last = pl.ds(0, 64), pl.ds(64, 64)
    z_up, z_down = at_z(up_z), at_z(down_z)
    r1 = send(rows_ref.at[first], gathered.at[0, first], row_ss.at[0], row_rs.at[0], z_up)
    l1 = send(rows_ref.at[last], gathered.at[1, last], row_ss.at[1], row_rs.at[1], z_down)
    a_up = send(aux.at[up_z], aux_in.at[0], aux_ss.at[0], aux_rs.at[0], z_up)
    a_down = send(aux.at[down_z], aux_in.at[1], aux_ss.at[1], aux_rs.at[1], z_down)
    a_far = send(aux.at[far_z], aux_relay, aux_ss.at[2], aux_rs.at[2], z_up)
    r2 = send(rows_ref.at[last], gathered.at[0, last], row_ss.at[2], row_rs.at[2], z_up)
    l2 = send(rows_ref.at[first], gathered.at[1, first], row_ss.at[3], row_rs.at[3], z_down)

    def places(info):
        at = jnp.broadcast_to(info[:8].reshape(8, 1, 128), (8, 32, 128)).reshape(256, 128)
        r, t = iota((256, 128), 0), iota((256, 128), 1)
        hit = (at == (r & 15).astype(F32)) & (((r >> 4) & 1) == (t >> 6))
        return jnp.where(hit, 1.0, 0.0)

    def info_of(k):
        return (aux[zh] if k == 0 else aux_in[k - 1]).astype(F32)

    mine = pl.ds(pl.multiple_of(yc * 32, 32), 32)

    def slab_send(k, src, dst, ss, rs):
        dst[k, mine] = src[k, mine]
        for d in range(1, 8):
            place = lax.rem(yc + d, 8)
            theirs = pl.ds(pl.multiple_of(place * 32, 32), 32)
            send(src.at[k, theirs], dst.at[k, mine], ss.at[k, d], rs.at[k, d], at_slab(place))

    def slab_wait(k, src, dst, ss, rs):
        for d in range(1, 8):
            place = lax.rem(yc + 8 - d, 8)
            theirs = pl.ds(pl.multiple_of(place * 32, 32), 32)
            copy(src.at[k, theirs], dst.at[k, theirs], ss.at[k, d], rs.at[k, d], at_slab(place)).wait_recv()

    def dispatch(k):
        rows = rows_ref[...] if k == 0 else gathered[k - 1]
        packed[k] = dot(places(info_of(k)).astype(BF16), rows).astype(BF16)
        slab_send(k, packed, arrived, go_ss, go_rs)

    def run_expert(k):
        slab_wait(k, packed, arrived, go_ss, go_rs)
        o = origin[k]
        dh = dot(arrived[k], wd[...], ((1,), (1,)))
        gate_grad = jnp.sum(dh * act_up[o], axis=1, keepdims=True)
        d_first = (dh * up_slope[o]).astype(BF16)
        d_second = (dh * act[o]).astype(BF16)
        rows = dot(d_first, wg[...], ((1,), (1,))) + dot(d_second, wu[...], ((1,), (1,)))
        back[k, :, :1024] = rows.astype(BF16)
        back[k, :, 1024:] = jnp.broadcast_to(gate_grad, (256, 128)).astype(BF16)
        slab_send(k, back, returned, ret_ss, ret_rs)

    def combine(k):
        slab_wait(k, back, returned, ret_ss, ret_rs)
        info = info_of(k)
        hit = places(info)
        gate = jnp.broadcast_to(info[8:].reshape(8, 1, 128), (8, 32, 128)).reshape(256, 128)
        weights = (hit * gate).T.astype(BF16)
        part = dot(weights, returned[k, :, :1024])
        gate_grad = hit * returned[k, :, 1024:].astype(F32)
        return part, jnp.sum(gate_grad.reshape(8, 32, 128), axis=1)

    dispatch(0)

    local[0].wait()
    local[1].wait()
    r, s = iota((256, 104), 0), iota((256, 104), 1)
    for o in range(4):
        gate_in, up_in = jnp.zeros((256, 704), F32), jnp.zeros((256, 704), F32)
        for n in range(2):
            real = (s == (r >> 5) * 13 + (r & 15)) & ((r & 15) < 13) & (((r >> 4) & 1) == n)
            spread = jnp.where(real, 1.0, 0.0).astype(BF16)
            gate_in += dot(spread, pre_gate[n * 4 + o])
            up_in += dot(spread, pre_up[n * 4 + o])
        sg = 1.0 / (1.0 + jnp.exp(-gate_in))
        active = gate_in * sg
        act[o] = active
        act_up[o] = active * up_in
        up_slope[o] = up_in * (sg * (1.0 + gate_in * (1.0 - sg)))
    for made in local[2:]:
        made.wait()
    run_expert(0)

    r1.wait_recv()
    r3 = send(gathered.at[0, first], gathered.at[2, first], row_ss.at[4], row_rs.at[4], z_up)
    l1.wait_recv()
    l3 = send(gathered.at[1, last], gathered.at[2, last], row_ss.at[5], row_rs.at[5], z_down)
    a_far.wait_recv()
    a_relay = send(aux_relay, aux_in.at[2], aux_ss.at[3], aux_rs.at[3], z_up)
    part, own_gate_grad = combine(0)
    own_part[...] = part
    pg_all[zh] = own_gate_grad

    a_up.wait_recv()
    r2.wait_recv()
    dispatch(1)
    a_down.wait_recv()
    l2.wait_recv()
    dispatch(2)
    run_expert(1)
    run_expert(2)
    part, gate_grad = combine(1)
    pg_out[0] = gate_grad
    p_down = send(pg_out.at[0], pg_all.at[zh], pg_ss.at[0], pg_rs.at[0], z_down)
    comb_out[0] = part[:64].astype(BF16)
    c_down = send(comb_out.at[0], comb_in.at[1, 0], comb_ss.at[0], comb_rs.at[0], z_down)
    relay_part[1] = part[64:]
    part, gate_grad = combine(2)
    pg_out[1] = gate_grad
    p_up = send(pg_out.at[1], pg_all.at[zh], pg_ss.at[1], pg_rs.at[1], z_up)
    comb_out[1] = part[64:].astype(BF16)
    c_up = send(comb_out.at[1], comb_in.at[0, 1], comb_ss.at[1], comb_rs.at[1], z_up)
    relay_part[0] = part[:64]

    a_relay.wait_recv()
    r3.wait_recv()
    l3.wait_recv()
    dispatch(3)
    run_expert(3)
    part, gate_grad = combine(3)
    pg_out[2] = gate_grad
    p_far = send(pg_out.at[2], pg_relay, pg_ss.at[2], pg_rs.at[2], z_up)
    comb_out[2] = part[:64].astype(BF16)
    comb_out[3] = part[64:].astype(BF16)
    f_up = send(comb_out.at[2], comb_mid.at[0], comb_ss.at[2], comb_rs.at[2], z_up)
    f_down = send(comb_out.at[3], comb_mid.at[1], comb_ss.at[3], comb_rs.at[3], z_down)
    p_far.wait_recv()
    p_relay = send(pg_relay, pg_all.at[down_z], pg_ss.at[3], pg_rs.at[3], z_up)

    p_down.wait_recv()
    p_up.wait_recv()
    p_relay.wait_recv()
    probability = probs[...]
    prob_grad = pg_all[...].reshape(32, 128)
    logit_grad = probability * (prob_grad - jnp.sum(probability * prob_grad, axis=0, keepdims=True))
    term = dot(logit_grad, hidden_ref[...].astype(F32), precision=PRECISE)
    for i in range(8):
        terms[i] = term[:, 128 * i : 128 * i + 128]

    def share(src, dst, ss, rs, me, count, to):
        made = []
        for d in range(1, count):
            place = lax.rem(me + d, count)
            made.append(send(src(place), dst.at[me], ss.at[d], rs.at[d], to(place)))
        return made

    def gather(src, dst, ss, rs, me, count, to):
        for d in range(1, count):
            place = lax.rem(me + count - d, count)
            copy(src(place), dst.at[place], ss.at[d], rs.at[d], to(place)).wait_recv()

    zl_args = (lambda place: terms.at[place], zl_in, zl_ss, zl_rs, zl, 8, lambda place: {"dp_0": place})
    x_args = (lambda place: stage_out.at[0], x_in, x_ss, x_rs, x, 4, lambda place: {"dp_1": place})
    slab_args = (lambda place: stage_out.at[1], slab_in, slab_ss, slab_rs, yc, 8, at_slab)
    sq_args = (lambda place: sq_out, sq_in, sq_ss, sq_rs, zl, 8, lambda place: {"dp_0": place})
    zl_in[zl] = terms[zl]
    share(*zl_args)

    f_up.wait_recv()
    comb_out[4] = (relay_part[0] + comb_mid[0].astype(F32)).astype(BF16)
    e_up = send(comb_out.at[4], comb_in.at[0, 0], comb_ss.at[4], comb_rs.at[4], z_up)
    f_down.wait_recv()
    comb_out[5] = (relay_part[1] + comb_mid[1].astype(F32)).astype(BF16)
    e_down = send(comb_out.at[5], comb_in.at[1, 1], comb_ss.at[5], comb_rs.at[5], z_down)

    gather(*zl_args)
    total = jnp.sum(zl_in[...], axis=0)
    stage_out[0] = total
    x_in[x] = total
    share(*x_args)
    padded = jnp.concatenate([logit_grad, jnp.zeros((96, 128), F32)], axis=0).T
    own_part[...] += dot(padded, rwt_ref[...], precision=PRECISE)
    gather(*x_args)
    total = jnp.sum(x_in[...], axis=0)
    stage_out[1] = total
    slab_in[yc] = total
    share(*slab_args)
    gather(*slab_args)
    total = jnp.sum(slab_in[...], axis=0)
    stage_out[2] = total
    h1 = send(stage_out.at[2], zh_in.at[0], zh_ss.at[0], zh_rs.at[0], at_z(zh + 1 - 2 * lax.rem(zh, 2)))
    h1.wait_recv()
    total = total + zh_in[0]
    stage_out[3] = total
    h2 = send(stage_out.at[3], zh_in.at[1], zh_ss.at[1], zh_rs.at[1], at_z(3 - zh))
    h2.wait_recv()
    total = total + zh_in[1]
    square = jnp.sum(jnp.sum(total * total, axis=1, keepdims=True), axis=0, keepdims=True)
    square = jnp.broadcast_to(square, (8, 128))
    sq_out[...] = square
    sq_in[zl] = square
    share(*sq_args)

    c_down.wait_recv()
    c_up.wait_recv()
    e_up.wait_recv()
    e_down.wait_recv()
    for half in range(2):
        at = pl.ds(64 * half, 64)
        both = comb_in[0, half].astype(F32) + comb_in[1, half].astype(F32)
        gx_ref[at] = (own_part[at] + both).astype(BF16)

    turned[...] = jnp.concatenate([total, jnp.zeros((96, 128), F32)], axis=0).T
    column = turned[pl.ds(pl.multiple_of(x * 32, 32), 32)]
    column = jnp.where(iota((32, 128), 1) == zh * 8 + yc, column, 0.0)
    column = jnp.sum(column, axis=1, keepdims=True)
    gather(*sq_args)
    square = jnp.sum(sq_in[...], axis=0)[:1, :1]
    ru_ref[...] = column * jnp.minimum(1.0, jnp.sqrt(1024 * 32 / (square + 1e-06)))
    for made in sent:
        made.wait_send()


def local(hidden, grad_out, router_weight, expert_ids, pre_gate, pre_up, w_gate, w_up, w_down):
    vmem, dma = pltpu.VMEM, pltpu.SemaphoreType.DMA
    wide = jnp.pad(router_weight, ((0, 0), (0, 96)))
    ids = jnp.pad(expert_ids.T, ((0, 2), (0, 0)))
    in_vmem, in_hbm = pl.BlockSpec(memory_space=pltpu.VMEM), pl.BlockSpec(memory_space=pl.ANY)
    return pl.pallas_call(
        kernel,
        out_shape=(jax.ShapeDtypeStruct((128, 1024), BF16), jax.ShapeDtypeStruct((32, 1), F32)),
        in_specs=[in_vmem] * 5 + [in_hbm] * 5,
        out_specs=(in_vmem, in_vmem),
        scratch_shapes=[
            vmem((8, 104, 704), BF16), vmem((8, 104, 704), BF16),
            vmem((1024, 704), BF16), vmem((1024, 704), BF16), vmem((704, 1024), BF16),
            vmem((3, 128, 1024), BF16), vmem((4, 16, 128), BF16), vmem((3, 16, 128), BF16), vmem((16, 128), BF16),
            vmem((4, 256, 1024), BF16), vmem((4, 256, 1024), BF16), vmem((4, 256, WIDE), BF16), vmem((4, 256, WIDE), BF16),
            vmem((4, 256, 704), F32), vmem((4, 256, 704), F32), vmem((4, 256, 704), F32), vmem((32, 128), F32),
            vmem((128, 1024), F32), vmem((2, 64, 1024), F32), vmem((6, 64, 1024), BF16), vmem((2, 64, 1024), BF16),
            vmem((2, 2, 64, 1024), BF16), vmem((3, 8, 128), F32), vmem((8, 128), F32), vmem((4, 8, 128), F32),
            vmem((8, 32, 128), F32), vmem((8, 32, 128), F32), vmem((4, 32, 128), F32), vmem((4, 32, 128), F32),
            vmem((8, 32, 128), F32), vmem((2, 32, 128), F32), vmem((8, 128), F32), vmem((8, 8, 128), F32),
            vmem((128, 128), F32),
            dma((5,)), dma((6,)), dma((6,)), dma((4,)), dma((4,)), dma((4, 8)), dma((4, 8)), dma((4, 8)), dma((4, 8)),
            dma((6,)), dma((6,)), dma((4,)), dma((4,)), dma((8,)), dma((8,)), dma((4,)), dma((4,)), dma((8,)), dma((8,)),
            dma((2,)), dma((2,)), dma((8,)), dma((8,)),
        ],
        compiler_params=pltpu.CompilerParams(collective_id=0, has_side_effects=True),
    )(
        grad_out, hidden, wide, wide.T, ids,
        pre_gate.reshape(8, 104, 704), pre_up.reshape(8, 104, 704), w_gate[0], w_up[0], w_down[0],
    )


def solution(mesh):
    torus = Mesh(mesh.devices.reshape(8, 4, 4, 4, 2), DP_EXPERT)
    return jax.shard_map(
        local,
        mesh=torus,
        in_specs=(
            P(DP_EXPERT, None),
            P(DP_EXPERT, None),
            P(),
            P(DP_EXPERT, None),
            P(DP, EXPERT, None, None),
            P(DP, EXPERT, None, None),
            P(EXPERT, None, None),
            P(EXPERT, None, None),
            P(EXPERT, None, None),
        ),
        out_specs=(P(DP_EXPERT, None), P(DP, EXPERT)),
        check_vma=False,
    )
```

```python
import jax
import jax.numpy as jnp
from jax import lax
from jax.experimental import pallas as pl
from jax.experimental.pallas import tpu as pltpu
from jax.sharding import Mesh
from jax.sharding import PartitionSpec as P

EXPERT = ("expert_0", "expert_1", "expert_2")
DP = ("dp_0", "dp_1")
DP_EXPERT = DP + EXPERT
PRECISE = lax.Precision.HIGHEST
F32 = jnp.float32
BF16 = jnp.bfloat16


def dot(a, b, dims=((1,), (0,)), precision=None):
    return lax.dot_general(a, b, (dims, ((), ())), preferred_element_type=F32, precision=precision)


def iota(shape, dim):
    return lax.broadcasted_iota(jnp.int32, shape, dim)


def kernel(
    rows_ref, hidden_ref, rw_ref, ids_ref, pre_gate_hbm, pre_up_hbm, wg_hbm, wu_hbm, wd_hbm,
    gx_ref, ru_ref,
    pre_gate, pre_up, wg, wu, wd, gathered, aux, aux_in, aux_relay,
    packed, arrived, back, returned, gate_out, gate_in, up_slope, act, act_up, probs,
    own_part, relay_part, comb_out, comb_mid, comb_in, pg_out, pg_early, pg_relay, pg_all,
    terms, x_in, slab_out, slab_in, tile_out, zl_in, zh_in, all_in, last_out, last_in,
    local_sem, row_ss, row_rs, aux_ss, aux_rs, go_ss, go_rs, ret_ss, ret_rs, gg_ss, gg_rs,
    comb_ss, comb_rs, pg_ss, pg_rs, zl_ss, zl_rs, x_ss, x_rs, slab_ss, slab_rs, zh_ss, zh_rs, all_ss, all_rs, last_ss, last_rs,
):
    zl, x = lax.axis_index("dp_0"), lax.axis_index("dp_1")
    zh, y, c = (lax.axis_index(a) for a in EXPERT)
    yc = y * 2 + c
    up_z, down_z, far_z = lax.rem(zh + 1, 4), lax.rem(zh + 3, 4), lax.rem(zh + 2, 4)
    origin = (zh, down_z, up_z, far_z)
    sent = []

    def at_z(z):
        return {"expert_0": z}

    def at_slab(place):
        return {"expert_1": place // 2, "expert_2": lax.rem(place, 2)}

    def copy(src, dst, ss, rs, to):
        return pltpu.make_async_remote_copy(
            src_ref=src, dst_ref=dst, send_sem=ss, recv_sem=rs,
            device_id=to, device_id_type=pl.DeviceIdType.MESH,
        )

    def send(*args):
        made = copy(*args)
        made.start()
        sent.append(made)
        return made

    local = [
        pltpu.make_async_copy(src, dst, local_sem.at[i])
        for i, (src, dst) in enumerate(
            ((pre_gate_hbm, pre_gate), (pre_up_hbm, pre_up), (wd_hbm, wd), (wg_hbm, wg), (wu_hbm, wu))
        )
    ]
    for made in local:
        made.start()
    barrier = pltpu.get_barrier_semaphore()
    meet = [at_z(up_z), at_z(down_z)]
    meet += [at_slab(lax.rem(yc + d, 8)) for d in range(1, 8)]
    meet += [{"dp_0": lax.rem(zl + d, 8)} for d in range(1, 8)]
    meet += [{"dp_1": lax.rem(x + d, 4)} for d in range(1, 4)]
    for to in meet:
        pl.semaphore_signal(barrier, inc=1, device_id=to, device_id_type=pl.DeviceIdType.MESH)

    logits = dot(rw_ref[...], hidden_ref[...].astype(F32), ((1,), (1,)), PRECISE)
    exponent = jnp.exp(logits)
    probability = exponent / jnp.sum(exponent, axis=0, keepdims=True)
    probs[...] = probability
    ids = ids_ref[...]
    expert = iota((32, 128), 0)
    chosen = jnp.zeros((32, 128), F32)
    for k in range(6):
        chosen += jnp.where(expert == ids[k : k + 1], 1.0, 0.0)
    r, t = iota((128, 128), 0), iota((128, 128), 1)
    earlier = jnp.where((r < t) & ((r >> 6) == (t >> 6)), 1.0, 0.0).astype(BF16)
    slot = jnp.where(chosen > 0.5, dot(chosen.astype(BF16), earlier), -1.0)
    for b in range(4):
        aux[b] = jnp.concatenate([slot[8 * b : 8 * b + 8], probability[8 * b : 8 * b + 8]], axis=0).astype(BF16)
    pl.semaphore_wait(barrier, len(meet))

    first, last = pl.ds(0, 64), pl.ds(64, 64)
    z_up, z_down = at_z(up_z), at_z(down_z)
    r1 = send(rows_ref.at[first], gathered.at[0, first], row_ss.at[0], row_rs.at[0], z_up)
    l1 = send(rows_ref.at[last], gathered.at[0, last], row_ss.at[1], row_rs.at[1], z_down)
    a_up = send(aux.at[up_z], aux_in.at[0], aux_ss.at[0], aux_rs.at[0], z_up)
    a_down = send(aux.at[down_z], aux_in.at[1], aux_ss.at[1], aux_rs.at[1], z_down)
    a_far = send(aux.at[far_z], aux_relay, aux_ss.at[2], aux_rs.at[2], z_up)
    r2 = send(rows_ref.at[last], gathered.at[1, last], row_ss.at[2], row_rs.at[2], z_up)
    l2 = send(rows_ref.at[first], gathered.at[1, first], row_ss.at[3], row_rs.at[3], z_down)

    def places(info):
        at = jnp.broadcast_to(info[:8].reshape(8, 1, 128), (8, 32, 128)).reshape(256, 128)
        r, t = iota((256, 128), 0), iota((256, 128), 1)
        hit = (at == (r & 15).astype(F32)) & (((r >> 4) & 1) == (t >> 6))
        return jnp.where(hit, 1.0, 0.0)

    def info_of(k):
        if k == 0:
            return aux[zh].astype(F32)
        if k == 3:
            return aux_in[2].astype(F32)
        return by_half(aux_in[k - 1].astype(F32), aux_in[2 - k].astype(F32))

    def by_half(a, b):
        return jnp.where(iota(a.shape, 1) < 64, a, b)

    def table_of(table, k):
        if k == 0 or k == 3:
            return table[origin[k]]
        return jnp.where((iota((256, 704), 0) & 16) == 0, table[origin[k]], table[origin[3 - k]])

    mine = pl.ds(pl.multiple_of(yc * 32, 32), 32)

    def slab_send(k, src, dst, ss, rs):
        dst[k, mine] = src[k, mine]
        for d in range(1, 8):
            place = lax.rem(yc + d, 8)
            theirs = pl.ds(pl.multiple_of(place * 32, 32), 32)
            send(src.at[k, theirs], dst.at[k, mine], ss.at[k, d], rs.at[k, d], at_slab(place))

    def slab_wait(k, src, dst, ss, rs):
        for d in range(1, 8):
            place = lax.rem(yc + 8 - d, 8)
            theirs = pl.ds(pl.multiple_of(place * 32, 32), 32)
            copy(src.at[k, theirs], dst.at[k, theirs], ss.at[k, d], rs.at[k, d], at_slab(place)).wait_recv()

    def dispatch(k):
        rows = rows_ref[...] if k == 0 else gathered[k - 1]
        packed[k] = dot(places(info_of(k)).astype(BF16), rows).astype(BF16)
        slab_send(k, packed, arrived, go_ss, go_rs)

    def run_expert(k):
        slab_wait(k, packed, arrived, go_ss, go_rs)
        dh = dot(arrived[k], wd[...], ((1,), (1,)))
        gate_grad = jnp.sum(dh * table_of(act_up, k), axis=1, keepdims=True)
        gate_out[k] = jnp.broadcast_to(gate_grad, (256, 128)).astype(BF16)
        slab_send(k, gate_out, gate_in, gg_ss, gg_rs)
        d_first = (dh * table_of(up_slope, k)).astype(BF16)
        d_second = (dh * table_of(act, k)).astype(BF16)
        back[k] = (dot(d_first, wg[...]) + dot(d_second, wu[...])).astype(BF16)
        slab_send(k, back, returned, ret_ss, ret_rs)

    def gate_part(k):
        slab_wait(k, gate_out, gate_in, gg_ss, gg_rs)
        gate_grad = places(info_of(k)) * gate_in[k].astype(F32)
        return jnp.sum(gate_grad.reshape(8, 32, 128), axis=1)

    def combine(k):
        info = info_of(k)
        gate = jnp.broadcast_to(info[8:].reshape(8, 1, 128), (8, 32, 128)).reshape(256, 128)
        weights = (places(info) * gate).T.astype(BF16)
        slab_wait(k, back, returned, ret_ss, ret_rs)
        return dot(weights, returned[k])

    dispatch(0)

    local[0].wait()
    local[1].wait()
    for o in range(4):
        saved_gate, saved_up = jnp.zeros((256, 704), F32), jnp.zeros((256, 704), F32)
        for n in range(2):
            start = n * 416 + o * 104
            lo = start // 128 * 128
            lanes = slice(lo, min(lo + 256, 832))
            r, s = iota((256, lanes.stop - lo), 0), iota((256, lanes.stop - lo), 1)
            real = (s == (r >> 5) * 13 + (r & 15) + (start - lo)) & ((r & 15) < 13) & (((r >> 4) & 1) == n)
            spread = jnp.where(real, 1.0, 0.0).astype(BF16)
            saved_gate += dot(spread, pre_gate[:, lanes], ((1,), (1,)))
            saved_up += dot(spread, pre_up[:, lanes], ((1,), (1,)))
        sg = 1.0 / (1.0 + jnp.exp(-saved_gate))
        active = saved_gate * sg
        act[o] = active
        act_up[o] = active * saved_up
        up_slope[o] = saved_up * (sg * (1.0 + saved_gate * (1.0 - sg)))
    for made in local[2:]:
        made.wait()
    run_expert(0)

    r1.wait_recv()
    r3 = send(gathered.at[0, first], gathered.at[2, first], row_ss.at[4], row_rs.at[4], z_up)
    l1.wait_recv()
    l3 = send(gathered.at[0, last], gathered.at[2, last], row_ss.at[5], row_rs.at[5], z_down)
    a_far.wait_recv()
    a_relay = send(aux_relay, aux_in.at[2], aux_ss.at[3], aux_rs.at[3], z_up)
    a_up.wait_recv()
    a_down.wait_recv()
    dispatch(1)
    pg_all[zh] = gate_part(0)
    own_part[...] = combine(0)
    run_expert(1)
    r2.wait_recv()
    l2.wait_recv()
    dispatch(2)
    pg_early[...] = gate_part(1)
    part = combine(1)
    comb_out[0] = part[:64].astype(BF16)
    c_down = send(comb_out.at[0], comb_in.at[1, 0], comb_ss.at[0], comb_rs.at[0], z_down)
    comb_out[1] = part[64:].astype(BF16)
    c_up = send(comb_out.at[1], comb_in.at[0, 1], comb_ss.at[1], comb_rs.at[1], z_up)
    run_expert(2)

    a_relay.wait_recv()
    r3.wait_recv()
    l3.wait_recv()
    dispatch(3)
    late, early = gate_part(2), pg_early[...]
    pg_out[0] = by_half(early, late)
    p_down = send(pg_out.at[0], pg_all.at[zh], pg_ss.at[0], pg_rs.at[0], z_down)
    pg_out[1] = by_half(late, early)
    p_up = send(pg_out.at[1], pg_all.at[zh], pg_ss.at[1], pg_rs.at[1], z_up)
    part = combine(2)
    relay_part[0] = part[:64]
    relay_part[1] = part[64:]
    run_expert(3)
    pg_out[2] = gate_part(3)
    p_far = send(pg_out.at[2], pg_relay, pg_ss.at[2], pg_rs.at[2], z_up)
    part = combine(3)
    comb_out[2] = part[:64].astype(BF16)
    comb_out[3] = part[64:].astype(BF16)

    def far_up(i):
        at = pl.ds(32 * i, 32)
        return send(comb_out.at[2, at], comb_mid.at[0, at], comb_ss.at[2 + i], comb_rs.at[2 + i], z_up)

    def far_down(i):
        at = pl.ds(32 * i, 32)
        return send(comb_out.at[3, at], comb_mid.at[1, at], comb_ss.at[4 + i], comb_rs.at[4 + i], z_down)

    def joined_up(i):
        at = pl.ds(32 * i, 32)
        comb_out[4, at] = (relay_part[0, at] + comb_mid[0, at].astype(F32)).astype(BF16)
        return send(comb_out.at[4, at], comb_in.at[0, 0, at], comb_ss.at[6 + i], comb_rs.at[6 + i], z_up)

    def joined_down(i):
        at = pl.ds(32 * i, 32)
        comb_out[5, at] = (relay_part[1, at] + comb_mid[1, at].astype(F32)).astype(BF16)
        return send(comb_out.at[5, at], comb_in.at[1, 1, at], comb_ss.at[8 + i], comb_rs.at[8 + i], z_down)

    f1_down = far_down(0)
    p_far.wait_recv()
    p_relay = send(pg_relay, pg_all.at[down_z], pg_ss.at[3], pg_rs.at[3], z_up)
    f1_up = far_up(0)
    f2_down = far_down(1)
    f2_up = far_up(1)

    p_down.wait_recv()
    p_up.wait_recv()
    p_relay.wait_recv()
    probability = probs[...]
    prob_grad = pg_all[...].reshape(32, 128)
    logit_grad = probability * (prob_grad - jnp.sum(probability * prob_grad, axis=0, keepdims=True))
    term = dot(logit_grad, hidden_ref[...].astype(F32), precision=PRECISE)
    for i in range(8):
        terms[i // 2, 32 * (i % 2) : 32 * (i % 2) + 32] = term[:, 128 * i : 128 * i + 128]

    def share(src, dst, ss, rs, me, count, to):
        made = []
        for d in range(1, count):
            place = lax.rem(me + d, count)
            made.append(send(src(place), dst.at[me], ss.at[d], rs.at[d], to(place)))
        return made

    def gather(src, dst, ss, rs, me, count, to):
        for d in range(1, count):
            place = lax.rem(me + count - d, count)
            copy(src(place), dst.at[place], ss.at[d], rs.at[d], to(place)).wait_recv()

    def zl_at(place):
        return {"dp_0": place}

    def x_at(place):
        return {"dp_1": place}

    x_args = (lambda place: terms.at[place], x_in, x_ss, x_rs, x, 4, x_at)
    slab_args = (lambda place: slab_out.at[place], slab_in, slab_ss, slab_rs, yc, 8, at_slab)
    zl_args = (lambda place: tile_out.at[0], zl_in, zl_ss, zl_rs, zl, 8, zl_at)
    all_args = (lambda place: tile_out.at[3], all_in, all_ss, all_rs, yc, 8, at_slab)
    last_args = (lambda place: last_out, last_in, last_ss, last_rs, x, 4, x_at)
    x_in[x] = terms[x]
    share(*x_args)
    turned = jnp.concatenate([logit_grad, jnp.zeros((96, 128), F32)], axis=0).T
    own_part[...] += dot(turned[:, :32], rw_ref[...], precision=PRECISE)
    gather(*x_args)
    slab_out[...] = jnp.sum(x_in[...], axis=0).reshape(8, 8, 128)
    slab_in[yc] = slab_out[yc]
    share(*slab_args)
    gather(*slab_args)
    tile = jnp.sum(slab_in[...], axis=0)
    tile_out[0] = tile
    zl_in[zl] = tile
    share(*zl_args)

    f1_up.wait_recv()
    e1_up = joined_up(0)
    f1_down.wait_recv()
    e1_down = joined_down(0)
    gather(*zl_args)
    tile = jnp.sum(zl_in[...], axis=0)
    tile_out[1] = tile
    h1 = send(tile_out.at[1], zh_in.at[0], zh_ss.at[0], zh_rs.at[0], at_z(zh + 1 - 2 * lax.rem(zh, 2)))
    f2_up.wait_recv()
    e2_up = joined_up(1)
    f2_down.wait_recv()
    e2_down = joined_down(1)
    h1.wait_recv()
    tile = tile + zh_in[0]
    tile_out[2] = tile
    h2 = send(tile_out.at[2], zh_in.at[1], zh_ss.at[1], zh_rs.at[1], at_z(3 - zh))
    h2.wait_recv()
    tile = tile + zh_in[1]
    tile_out[3] = tile
    all_in[yc] = tile
    share(*all_args)
    gather(*all_args)
    tiles = jnp.sum(all_in[...] * all_in[...], axis=0)
    square = jnp.sum(jnp.sum(tiles, axis=1, keepdims=True), axis=0, keepdims=True)
    last_out[:8] = all_in[lax.rem(zl, 2) * 4 + zh]
    last_out[8:] = jnp.broadcast_to(square, (8, 128))
    last_in[x] = last_out[...]
    share(*last_args)

    for made in (c_down, c_up, e1_up, e1_down, e2_up, e2_down):
        made.wait_recv()
    for half in range(2):
        at = pl.ds(64 * half, 64)
        both = comb_in[0, half].astype(F32) + comb_in[1, half].astype(F32)
        gx_ref[at] = (own_part[at] + both).astype(BF16)

    gather(*last_args)
    tile = last_in[zl // 2][:8]
    column = jnp.where(iota((8, 128), 0) == yc, tile, 0.0)
    column = jnp.sum(column, axis=0, keepdims=True)
    column = sum(jnp.where(x == i, column[:, 32 * i : 32 * i + 32], 0.0) for i in range(4))
    square = jnp.sum(last_in[...], axis=0)[8:9, :1]
    ru_ref[...] = column * jnp.minimum(1.0, jnp.sqrt(1024 * 32 / (square + 1e-06)))
    for made in sent:
        made.wait_send()


def local(hidden, grad_out, router_weight, expert_ids, pre_gate, pre_up, w_gate, w_up, w_down):
    vmem, dma = pltpu.VMEM, pltpu.SemaphoreType.DMA
    in_vmem, in_hbm = pl.BlockSpec(memory_space=pltpu.VMEM), pl.BlockSpec(memory_space=pl.ANY)
    grad_x, update = pl.pallas_call(
        kernel,
        out_shape=(jax.ShapeDtypeStruct((128, 1024), BF16), jax.ShapeDtypeStruct((1, 32), F32)),
        in_specs=[in_vmem] * 4 + [in_hbm] * 5,
        out_specs=(in_vmem, in_vmem),
        scratch_shapes=[
            vmem((704, 832), BF16), vmem((704, 832), BF16),
            vmem((704, 1024), BF16), vmem((704, 1024), BF16), vmem((704, 1024), BF16),
            vmem((3, 128, 1024), BF16), vmem((4, 16, 128), BF16), vmem((3, 16, 128), BF16), vmem((16, 128), BF16),
            vmem((4, 256, 1024), BF16), vmem((4, 256, 1024), BF16), vmem((4, 256, 1024), BF16), vmem((4, 256, 1024), BF16),
            vmem((4, 256, 128), BF16), vmem((4, 256, 128), BF16),
            vmem((4, 256, 704), F32), vmem((4, 256, 704), F32), vmem((4, 256, 704), F32), vmem((32, 128), F32),
            vmem((128, 1024), F32), vmem((2, 64, 1024), F32), vmem((6, 64, 1024), BF16), vmem((2, 64, 1024), BF16),
            vmem((2, 2, 64, 1024), BF16), vmem((3, 8, 128), F32), vmem((8, 128), F32), vmem((8, 128), F32), vmem((4, 8, 128), F32),
            vmem((4, 64, 128), F32), vmem((4, 64, 128), F32), vmem((8, 8, 128), F32), vmem((8, 8, 128), F32),
            vmem((4, 8, 128), F32), vmem((8, 8, 128), F32), vmem((2, 8, 128), F32), vmem((8, 8, 128), F32),
            vmem((16, 128), F32), vmem((4, 16, 128), F32),
            dma((5,)), dma((6,)), dma((6,)), dma((4,)), dma((4,)), dma((4, 8)), dma((4, 8)), dma((4, 8)), dma((4, 8)),
            dma((4, 8)), dma((4, 8)), dma((10,)), dma((10,)), dma((4,)), dma((4,)), dma((8,)), dma((8,)), dma((4,)), dma((4,)), dma((8,)), dma((8,)),
            dma((2,)), dma((2,)), dma((8,)), dma((8,)), dma((4,)), dma((4,)),
        ],
        compiler_params=pltpu.CompilerParams(collective_id=0, has_side_effects=True),
    )(
        grad_out, hidden, router_weight.T, expert_ids.T,
        pre_gate[0, 0].T, pre_up[0, 0].T, w_gate[0].T, w_up[0].T, w_down[0],
    )
    return grad_x, update.reshape(32, 1)


def solution(mesh):
    torus = Mesh(mesh.devices.reshape(8, 4, 4, 4, 2), DP_EXPERT)
    return jax.shard_map(
        local,
        mesh=torus,
        in_specs=(
            P(DP_EXPERT, None),
            P(DP_EXPERT, None),
            P(),
            P(DP_EXPERT, None),
            P(DP, EXPERT, None, None),
            P(DP, EXPERT, None, None),
            P(EXPERT, None, None),
            P(EXPERT, None, None),
            P(EXPERT, None, None),
        ),
        out_specs=(P(DP_EXPERT, None), P(DP, EXPERT)),
        check_vma=False,
    )
```
